32 devices in a mesh: dp: 1 (over z), ep: 32 (over x, y, core).
Axes of the slice: x: 4, y: 4, z: 1, core: 2. Of those that a mesh axis runs over, the one named last changes fastest.
The devices are a block of a 4x4x8 slice.
Arguments:
- x: bfloat16 [1, 32, 256, 4096], P('dp', 'ep')
- expert: int32 [1, 32, 256, 8], P('dp', 'ep')
- slot: int32 [1, 32, 256, 8], P('dp', 'ep')
- gate: float32 [1, 32, 256, 8], P('dp', 'ep')
- w_gate: bfloat16 [64, 4096, 1536], P('ep')
- w_up: bfloat16 [64, 4096, 1536], P('ep')
- w_down: bfloat16 [64, 1536, 4096], P('ep')
Outputs:
- y: bfloat16 [1, 32, 256, 4096], P('dp', 'ep')
All inputs are finite; a program needn't handle non-finite values.
Results may differ from the reference program's by a relative error of at most 0.009.
Values are sent between devices in bfloat16 or wider.
A program may use at most 768 MiB of HBM per device.

```python
import jax
import jax.numpy as jnp

MEMBERS = 32
TOKENS = 256
D = 4096
FF = 1536
TOP = 8
EXPERTS = 64
SLOTS = 5 * TOKENS * TOP // (4 * EXPERTS)


def setup_inputs(seed: int = 0, part: int = 0) -> dict:
    own, k1, k2, k3, k4, k5, k6 = jax.random.split(jax.random.key(seed), 7)
    kx, ke, kl, kg = jax.random.split(jax.random.fold_in(own, part), 4)
    devices = (1, MEMBERS)
    place = jax.random.permutation(kl, jnp.arange(EXPERTS, dtype=jnp.uint32))
    slow = ((EXPERTS + (9 * place) % EXPERTS) << ((9 * place) // EXPERTS)) // EXPERTS
    wait = (jax.random.bits(ke, (*devices, TOKENS, EXPERTS), jnp.uint32) >> 10) * slow
    expert = jnp.argsort(wait, axis=-1)[..., :TOP].astype(jnp.int32)
    chosen = jax.nn.one_hot(expert, EXPERTS, dtype=jnp.int32)
    in_line = jnp.cumsum(chosen.reshape(*devices, TOKENS * TOP, EXPERTS), axis=2) - 1
    slot = jnp.sum(in_line.reshape(chosen.shape) * chosen, axis=-1)

    def one(key, rows, columns):
        return (jax.random.normal(key, (rows, columns), jnp.float32) * rows**-0.5).astype(jnp.bfloat16)

    def weights(key, rows, columns):
        return jax.lax.map(lambda k: one(k, rows, columns), jax.random.split(key, EXPERTS))

    return {
        "x": jax.random.normal(kx, (*devices, TOKENS, D), jnp.float32).astype(jnp.bfloat16),
        "expert": expert,
        "slot": slot,
        "gate": jax.nn.softmax(jax.random.normal(kg, expert.shape, jnp.float32)),
        "w_gate": weights(k1, D, FF),
        "w_up": weights(k2, D, FF),
        "w_down": weights(k3, FF, D),
    }


def einsum(form, a, b):
    return jnp.einsum(form, a.astype(jnp.float32), b.astype(jnp.float32))


def reference(x, expert, slot, gate, w_gate, w_up, w_down):
    to_expert = jax.nn.one_hot(expert, EXPERTS, dtype=jnp.bfloat16)
    to_slot = jax.nn.one_hot(slot, SLOTS, dtype=jnp.bfloat16)
    weighted = to_expert * gate[..., None].astype(jnp.bfloat16)
    dispatch = einsum("abtke,abtkc->abtec", to_expert, to_slot).astype(jnp.bfloat16)
    combine = einsum("abtke,abtkc->abtec", weighted, to_slot).astype(jnp.bfloat16)
    z = einsum("abtec,abtd->aebcd", dispatch, x).astype(jnp.bfloat16)
    h = jax.nn.silu(einsum("aebcd,edf->aebcf", z, w_gate))
    h = (h * einsum("aebcd,edf->aebcf", z, w_up)).astype(jnp.bfloat16)
    out = einsum("aebcf,efd->aebcd", h, w_down).astype(jnp.bfloat16)
    y = einsum("abtec,aebcd->abtd", combine, out)
    return y.astype(jnp.bfloat16)
```

```python
import functools

import jax
import jax.numpy as jnp
from jax import lax
from jax.experimental import pallas as pl
from jax.experimental.pallas import tpu as pltpu
from jax.sharding import PartitionSpec as P

MESH = pl.DeviceIdType.MESH
F32, BF16 = jnp.float32, jnp.bfloat16
HC = 256
NT = 512
KINDS = ((0, 0), (0, -1), (0, 1), (-1, 0), (-1, 1), (1, 0), (1, -1))
ROWS = (-1, 0, 1)
TWO = range(2)
SIG = (1, -1)
FP, FM, SP, SM, HERE = (1, 0), (-1, 0), (0, 1), (0, -1), (0, 0)
OTHER, FAR = 1, 2
rem, div = lax.rem, lax.div


def kind(r, d):
    return KINDS.index((r, d))


def place(n):
    me = lax.axis_index("ep")
    c, chip = rem(me, 2), div(me, 2)
    a, b = div(chip, n), rem(chip, n)
    f, s = a * (1 - c) + b * c, b * (1 - c) + a * c

    def chip_at(at):
        ff, ss = rem(f + at[0] + n, n), rem(s + at[1] + n, n)
        return (ff * (1 - c) + ss * c) * n + ss * (1 - c) + ff * c

    def dev(at, other=0):
        return {"ep": chip_at(at) * 2 + (1 - c if other else c)}

    return dev, chip_at


def signal(sem, device):
    pl.semaphore_signal(sem, inc=1, device_id=device, device_id_type=MESH)


def greet(devices):
    barrier = pltpu.get_barrier_semaphore()
    for d in devices:
        signal(barrier, d)
    pl.semaphore_wait(barrier, len(devices))


def times(s, at=SP):
    return tuple(s * v for v in at)


def columns(j, h):
    return pl.ds(pl.multiple_of((2 * j + h) * HC, HC), HC)


def dot(a, b):
    return jnp.dot(a, b, preferred_element_type=F32)


def up_kernel(
    n, chunks, top, x_ref, meta_ref, lid_ref, wg_ref, wu_ref, h_ref, near_ref,
    row, nxt, zbuf, leaf, rel, part, p_ref, metas, wbuf, acc, hst, send, recv, msend, mrecv, msem, xsem, wsem, hsem, cred,
):
    dev, chip_at = place(n)
    c40 = p_ref.shape[2] // 4
    w = n * c40
    partner = dev(HERE, OTHER)
    sources = [(df, ds) for df in range(n) for ds in ROWS if (df, ds) != HERE]
    greet([dev(at) for at in sources] + [dev(at, OTHER) for at in (FP, FM, SP, SM)] + [partner])

    def remote(src, dst, s, r, to):
        return pltpu.make_async_remote_copy(
            src_ref=src, dst_ref=dst, send_sem=s, recv_sem=r, device_id=to, device_id_type=MESH
        )

    def copy(i, j, src, dst, to):
        m = rem(j, 3)
        return remote(src, dst, send.at[m, i], recv.at[m, i], to)

    tell = [
        remote(meta_ref, metas.at[-df % n, 1 - ds], msend.at[i], mrecv.at[i], dev((df, ds)))
        for i, (df, ds) in enumerate(sources)
    ]
    own = pltpu.make_async_copy(meta_ref, metas.at[0, 1], msem.at[0])

    def ring(j):
        r = row.at[rem(j, 3)]
        return [copy(h, j, r.at[:, 0], r.at[:, -SIG[h] % n], dev(times(SIG[h], FP))) for h in TWO]

    def onward(j):
        r = row.at[rem(j, 3)]
        return [copy(2 + h, j, r.at[h, -SIG[h] % n], r.at[h, FAR], dev(times(SIG[h], FP))) for h in TWO]

    def raw(j):
        r, t = row.at[rem(j, 3)], nxt.at[rem(j, 2)]
        return [copy(4 + h, j, r.at[h], t.at[h], dev(times(SIG[h]))) for h in TWO]

    def leaves(j, h):
        z, q = zbuf.at[rem(j, 3)], leaf.at[rem(j, 2)]
        return [copy(6 + 2 * h + o, j, q.at[h, o], z.at[h, o, SIG[h] % n], dev(times(-SIG[h]), o)) for o in TWO]

    def relays(j, h):
        z, q = zbuf.at[rem(j, 3)], rel.at[rem(j, 2)]
        return [copy(10 + 2 * h + o, j, q.at[h, o], z.at[h, o, FAR], dev(times(SIG[h]), o)) for o in TWO]

    def mine(j):
        z, q = zbuf.at[rem(j, 3)], part.at[rem(j, 2)]
        return copy(14, j, q.at[0], z.at[:, 1, 0], partner)

    def mine_next(j, h):
        z, q = zbuf.at[rem(j, 3)], part.at[rem(j, 2)]
        return copy(15 + h, j, q.at[1, h], z.at[h, 1, -SIG[h] % n], partner)

    def load(j):
        r, s = row.at[rem(j, 3)], xsem.at[rem(j, 2)]
        return [pltpu.make_async_copy(x_ref.at[:, columns(j, h)], r.at[h, 0], s.at[h]) for h in TWO]

    def weights(i, m, e):
        rows = pl.ds(pl.multiple_of(i * 2 * HC, HC), 2 * HC)
        return pltpu.make_async_copy((wg_ref, wu_ref)[m].at[e, rows], wbuf.at[m, e], wsem.at[m, e])

    def into_slots(k, src, put):
        for pair in TWO:
            r = [dot(p_ref[k, 2 * pair + i], src[2 * pair + i]) for i in TWO]
            for o in TWO:
                for e in TWO:
                    cut = slice((2 * o + e) * c40, (2 * o + e + 1) * c40)
                    v = jnp.concatenate([r[0][cut], r[1][cut]], axis=0).astype(BF16)
                    put(o, e, pl.ds(2 * pair * c40, 2 * c40), v)

    def matmul(i, m, e):
        weights(i, m, e).wait()
        tiles = acc.shape[-1] // NT
        z = zbuf.at[rem(i, 3)]

        def tile(t, carry):
            side, cols = div(t, tiles), pl.ds(pl.multiple_of(rem(t, tiles) * NT, NT), NT)
            a = jnp.concatenate([z[h, side, :, e].reshape(n * w, HC) for h in TWO], axis=1)
            acc[m, e, side, :, cols] += dot(a, wbuf[m, e, :, cols])
            return carry

        lax.fori_loop(0, 2 * tiles, tile, 0)

        @pl.when(i + 1 < chunks)
        def _():
            weights(i + 1, m, e).start()

    for d in load(0) + [own] + tell:
        d.start()
    for m in TWO:
        for e in TWO:
            weights(0, m, e).start()

    def tables():
        own.wait()
        for d in tell:
            d.wait_recv()
        lid = lid_ref[...]

        def source(g, carry):
            for k, (r, d) in enumerate(KINDS):
                first = (chip_at((0, d)) * 4 * c40).astype(F32)
                hit = None
                for j in range(top):
                    same = (metas[g, 1 + r, j : j + 1, :] - first) == lid
                    hit = same if hit is None else hit | same
                p_ref[k, g] = jnp.where(hit, 1.0, 0.0).astype(BF16)
            return carry

        lax.fori_loop(0, n, source, 0)
        for d in tell:
            d.wait_send()
        save = pltpu.make_async_copy(metas, near_ref, msem.at[1])
        save.start()
        acc[...] = jnp.zeros_like(acc)
        save.wait()

    def step(k, carry):
        @pl.when(k >= 2)
        def _():
            for i in range(7):
                pl.semaphore_wait(cred.at[i], 1)

        @pl.when(k < chunks)
        def _():
            for d in load(k):
                d.wait()
            for d in ring(k):
                d.start()

        @pl.when(k + 1 < chunks)
        def _():
            for d in load(k + 1):
                d.start()

        j, i = k - 1, k - 2
        travels, multiplies = (k >= 1) & (k <= chunks), k >= 2

        @pl.when(travels)
        def _():
            for d in onward(j):
                d.wait_recv()
            for d in raw(j):
                d.start()
            m3, m2 = rem(j, 3), rem(j, 2)
            for h in TWO:

                def put(o, e, rows, v):
                    leaf[m2, h, o, e, rows, :] = v

                into_slots(kind(0, -SIG[h]), row.at[m3, h], put)
                for d in leaves(j, h):
                    d.start()
            for h in TWO:

                def put(o, e, rows, v):
                    if o == 0:
                        zbuf[m3, h, 0, 0, e, rows, :] = v
                    else:
                        part[m2, 0, h, e, rows, :] = v

                into_slots(kind(*HERE), row.at[m3, h], put)
            mine(j).start()

        @pl.when(k == 0)
        def _():
            tables()

        @pl.when(multiplies)
        def _():
            for h in TWO:
                for d in leaves(i, h) + relays(i, h) + [mine_next(i, h)]:
                    d.wait_recv()
            mine(i).wait_recv()
            matmul(i, 0, 0)

        @pl.when(k < chunks)
        def _():
            for d, e in zip(ring(k), onward(k)):
                d.wait_recv()
                e.start()

        @pl.when(multiplies)
        def _():
            matmul(i, 0, 1)

        @pl.when(travels)
        def _():
            m3, m2 = rem(j, 3), rem(j, 2)
            for h in TWO:
                raw(j)[h].wait_recv()

                def put(o, e, rows, v):
                    rel[m2, h, o, e, rows, :] = v

                into_slots(kind(-SIG[h], SIG[h]), nxt.at[m2, h], put)
                for d in relays(j, h):
                    d.start()
            for h in TWO:

                def put(o, e, rows, v):
                    if o == 0:
                        zbuf[m3, h, 0, -SIG[h] % n, e, rows, :] = v
                    else:
                        part[m2, 1, h, e, rows, :] = v

                into_slots(kind(-SIG[h], 0), nxt.at[m2, h], put)
                mine_next(j, h).start()

        @pl.when(multiplies)
        def _():
            for e in TWO:
                matmul(i, 1, e)

        @pl.when(travels)
        def _():
            for d in ring(j) + onward(j) + raw(j) + leaves(j, 0) + leaves(j, 1) + [mine(j)]:
                d.wait_send()

        @pl.when(multiplies)
        def _():
            for h in TWO:
                for d in relays(i, h) + [mine_next(i, h)]:
                    d.wait_send()

        @pl.when(k < chunks)
        def _():
            to = [dev(at) for at in (FM, FP, SM, SP)] + [dev(at, OTHER) for at in (FM, FP)] + [partner]
            for q, d in enumerate(to):
                signal(cred.at[q], d)

        return carry

    lax.fori_loop(0, chunks + 2, step, 0)

    def save(t):
        e, side, soff = div(t, 2 * n), div(rem(t, 2 * n), n), rem(t, n)
        return pltpu.make_async_copy(hst.at[rem(t, 2)], h_ref.at[e, side, soff], hsem.at[rem(t, 2)])

    blocks = 4 * n

    def gated(t, carry):
        e, side, soff = div(t, 2 * n), div(rem(t, 2 * n), n), rem(t, n)
        rows = pl.ds(pl.multiple_of(soff * w, w), w)

        @pl.when(t >= 2)
        def _():
            save(t - 2).wait()

        hst[rem(t, 2)] = (jax.nn.silu(acc[0, e, side, rows, :]) * acc[1, e, side, rows, :]).astype(BF16)
        save(t).start()
        return carry

    lax.fori_loop(0, blocks, gated, 0)
    for t in (blocks - 2, blocks - 1):
        save(t).wait()


def down_kernel(
    n, chunks, top, h_ref, wd_ref, metas, lid_ref, y_ref,
    hbuf, wbuf, c_ref, ob, orl, olf, opt, yrow, f2r, fr, yst, fst, fin, ysum, y0, yo, send, recv, wsem, hsem, ysem, cred,
):
    dev, chip_at = place(n)
    rows2 = c_ref.shape[3] // 4
    w = hbuf.shape[3]
    partner = dev(HERE, OTHER)
    greet([dev(at, o) for at in (FP, FM, SP, SM) for o in TWO] + [partner])

    def m4(j):
        return rem(j, 4)

    def copy(i, j, src, dst, to):
        m = m4(j)
        return pltpu.make_async_remote_copy(
            src_ref=src, dst_ref=dst, send_sem=send.at[m, i], recv_sem=recv.at[m, i], device_id=to, device_id_type=MESH
        )

    def to_relay(j, h):
        o, q = ob.at[m4(j)], orl.at[m4(j)]
        to = dev(times(-SIG[h])), dev(times(-SIG[h], FP), OTHER)
        return [copy(2 * v + h, j, o.at[h, v, FAR], q.at[h, v], to[v]) for v in TWO]

    def to_root(j, h):
        o, q = ob.at[m4(j)], olf.at[m4(j)]
        to = dev(times(SIG[h])), dev(times(SIG[h], FP), OTHER)
        return [copy(4 + 2 * v + h, j, o.at[h, v, SIG[h] % n], q.at[h, v], to[v]) for v in TWO]

    def mine(j, h):
        o, q = ob.at[m4(j)], opt.at[m4(j)]
        ends = ((0, 8 + h, 0), (1, 10 + h, -SIG[h] % n))
        return [copy(i, j, o.at[h, 1, s], q.at[v, h], partner) for v, i, s in ends]

    def relayed(j):
        return [copy(12 + h, j, yst.at[rem(j, 2), h], yrow.at[m4(j), h], dev(times(-SIG[h]))) for h in TWO]

    def far(j):
        return [copy(14 + h, j, fst.at[rem(j, 2), h], f2r.at[m4(j), h], dev(times(-SIG[h], FP))) for h in TWO]

    def near(j):
        return [copy(16 + h, j, fin.at[rem(j, 2), h], fr.at[m4(j), h], dev(times(-SIG[h], FP))) for h in TWO]

    def firsts(j):
        return [d for h in TWO for d in to_relay(j, h) + to_root(j, h) + mine(j, h)]

    def weights(j):
        b, s = wbuf.at[rem(j, 2)], wsem.at[rem(j, 2)]
        return [pltpu.make_async_copy(wd_ref.at[e, :, columns(j, h)], b.at[h, e], s.at[h, e]) for h in TWO for e in TWO]

    def save(j):
        b = yo.at[rem(j, 2)]
        return [pltpu.make_async_copy(b.at[h], y_ref.at[:, columns(j, h)], ysem.at[h]) for h in TWO]

    def hidden(e, side):
        return pltpu.make_async_copy(h_ref.at[e, side], hbuf.at[e, side], hsem.at[e, side])

    def tokens(k, g, ours, theirs):
        cut = pl.ds((g // 2) * rows2, rows2)
        v = jnp.concatenate([o[e, cut, :] for o in (ours, theirs) for e in TWO], axis=0)
        return dot(c_ref[k, g], v)

    for side in TWO:
        for e in TWO:
            hidden(e, side).start()
    for d in weights(0):
        d.start()

    def tables():
        def source(g, carry):
            lid = lid_ref[rem(g, 2)]
            for r in ROWS:
                meta = metas[g, 1 + r].T
                for d in ROWS:
                    if (r, d) in KINDS:
                        first = (chip_at((0, d)) * 2 * rows2).astype(F32)
                        v = jnp.zeros(c_ref.shape[2:], F32)
                        for j in range(top):
                            same = (meta[:, j : j + 1] - first) == lid
                            v = jnp.where(same, meta[:, top + j : top + j + 1], v)
                        c_ref[kind(r, d), g] = v.astype(BF16)
            return carry

        lax.fori_loop(0, n, source, 0)

    def step(k, carry):
        @pl.when(k >= 2)
        def _():
            for i in range(7):
                pl.semaphore_wait(cred.at[i], 1)

        @pl.when((k >= 2) & (k <= chunks + 1))
        def _():
            j = k - 2
            m, m2 = m4(j), rem(j, 2)
            for d in to_root(j, 0) + to_root(j, 1) + [mine(j, h)[0] for h in TWO] + relayed(j):
                d.wait_recv()
            for h in TWO:
                s = SIG[h]
                for g in (2, 1, 3, 0):
                    v = tokens(kind(*HERE), g, ob.at[m, h, 0, 0], opt.at[m, 0, h])
                    v += tokens(kind(0, -s), g, olf.at[m, h, 0], olf.at[m, h, 1])
                    v += yrow[m, h, g].astype(F32)
                    if g == FAR:
                        fst[m2, h] = v.astype(BF16)
                        far(j)[h].start()
                    elif g == 0:
                        y0[m2, h] = v
                    else:
                        ysum[h, g // 2] = v

        @pl.when((k >= 1) & (k <= chunks))
        def _():
            j = k - 1
            m = m4(j)
            for h in TWO:
                s = SIG[h]
                for d in to_relay(j, h) + mine(j, h)[1:]:
                    d.wait_recv()
                for g in range(n):
                    v = tokens(kind(-s, 0), g, ob.at[m, h, 0, -s % n], opt.at[m, 1, h])
                    v += tokens(kind(-s, s), g, orl.at[m, h, 0], orl.at[m, h, 1])
                    yst[rem(j, 2), h, g] = v.astype(BF16)
                relayed(j)[h].start()

        @pl.when(k + 1 < chunks)
        def _():
            for d in weights(k + 1):
                d.start()

        @pl.when(k < chunks)
        def _():
            for d in weights(k):
                d.wait()
            m = m4(k)
            for h in TWO:
                for side in TWO:
                    for e in TWO:
                        if h == 0:

                            @pl.when(k == 0)
                            def _():
                                hidden(e, side).wait()

                        a = hbuf[e, side].reshape(n * w, hbuf.shape[4])
                        v = dot(a, wbuf[rem(k, 2), h, e]).astype(BF16)
                        ob[m, h, side, :, e] = v.reshape(n, w, HC)
                    to_relay(k, h)[side].start()
                    to_root(k, h)[side].start()
                for d in mine(k, h):
                    d.start()

        @pl.when(k == 0)
        def _():
            tables()

        @pl.when(k >= 3)
        def _():
            j = k - 3
            m, m2 = m4(j), rem(j, 2)
            for d in near(j):
                d.wait_recv()
            for h in TWO:
                yo[m2, h] = (y0[m2, h] + fr[m, 0, h].astype(F32) + fr[m, 1, h].astype(F32)).astype(BF16)
            for d in save(j):
                d.start()

        @pl.when((k >= 2) & (k <= chunks + 1))
        def _():
            j = k - 2
            m, m2 = m4(j), rem(j, 2)
            for h in TWO:
                far(j)[h].wait_recv()
                g = 1 - h
                fin[m2, h, h] = (ysum[h, g] + f2r[m, h].astype(F32)).astype(BF16)
                fin[m2, h, 1 - h] = ysum[1 - h, g].astype(BF16)
                near(j)[h].start()

        @pl.when((k >= 1) & (k <= chunks))
        def _():
            for d in firsts(k - 1):
                d.wait_send()

        @pl.when((k >= 2) & (k <= chunks + 1))
        def _():
            for d in relayed(k - 2):
                d.wait_send()

        @pl.when(k >= 3)
        def _():
            for d in far(k - 3) + near(k - 3):
                d.wait_send()
            for d in save(k - 3):
                d.wait()

        @pl.when(k < chunks + 1)
        def _():
            to = [dev(at) for at in (FM, FP, SM, SP)] + [dev(at, OTHER) for at in (SM, SP)] + [partner]
            for q, d in enumerate(to):
                signal(cred.at[q], d)

        return carry

    lax.fori_loop(0, chunks + 3, step, 0)


ANY = pl.BlockSpec(memory_space=pl.ANY)
VMEM = pl.BlockSpec(memory_space=pltpu.VMEM)
DMA, REGULAR = pltpu.SemaphoreType.DMA, pltpu.SemaphoreType.REGULAR


def bf16(*shape):
    return pltpu.VMEM(shape, BF16)


def f32(*shape):
    return pltpu.VMEM(shape, F32)


def params(i):
    return pltpu.CompilerParams(collective_id=i, has_side_effects=True, vmem_limit_bytes=66_500_000)


def up(n, slots, top, x, meta, lid, wg, wu):
    t, d = x.shape
    w, ff = n * slots, wg.shape[-1]
    slot_rows = bf16(2, 2, 2, 2, w, HC)
    return pl.pallas_call(
        functools.partial(up_kernel, n, d // (2 * HC), top),
        out_shape=(
            jax.ShapeDtypeStruct((2, 2, n, w, ff), BF16),
            jax.ShapeDtypeStruct((n, len(ROWS), *meta.shape), F32),
        ),
        in_specs=[ANY, VMEM, VMEM, ANY, ANY],
        out_specs=(ANY, ANY),
        scratch_shapes=[
            bf16(3, 2, n, t, HC),
            bf16(2, 2, n, t, HC),
            bf16(3, 2, 2, n, 2, w, HC),
            slot_rows,
            slot_rows,
            slot_rows,
            bf16(len(KINDS), n, 4 * slots, t),
            f32(n, len(ROWS), *meta.shape),
            bf16(2, 2, 2 * HC, ff),
            f32(2, 2, 2, n * w, ff),
            bf16(2, w, ff),
            DMA((3, 17)),
            DMA((3, 17)),
            DMA((3 * n - 1,)),
            DMA((3 * n - 1,)),
            DMA((2,)),
            DMA((2, 2)),
            DMA((2, 2)),
            DMA((2,)),
            REGULAR((7,)),
        ],
        compiler_params=params(0),
        name="up",
    )(x, meta, lid, wg, wu)


def down(n, slots, top, h, wd, metas, lid):
    d = wd.shape[-1]
    t, w, ff = metas.shape[-1], n * slots, h.shape[-1]
    rows = bf16(4, 2, 2, 2, w, HC)
    return pl.pallas_call(
        functools.partial(down_kernel, n, d // (2 * HC), top),
        out_shape=jax.ShapeDtypeStruct((t, d), BF16),
        in_specs=[ANY, ANY, VMEM, VMEM],
        out_specs=ANY,
        scratch_shapes=[
            bf16(2, 2, n, w, ff),
            bf16(2, 2, 2, ff, HC),
            bf16(len(KINDS), n, t, 8 * slots),
            bf16(4, 2, 2, n, 2, w, HC),
            rows,
            rows,
            rows,
            bf16(4, 2, n, t, HC),
            bf16(4, 2, t, HC),
            bf16(4, 2, 2, t, HC),
            bf16(2, 2, n, t, HC),
            bf16(2, 2, t, HC),
            bf16(2, 2, 2, t, HC),
            f32(2, 2, t, HC),
            f32(2, 2, t, HC),
            bf16(2, 2, t, HC),
            DMA((4, 18)),
            DMA((4, 18)),
            DMA((2, 2, 2)),
            DMA((2, 2)),
            DMA((2,)),
            REGULAR((7,)),
        ],
        compiler_params=params(1),
        name="down",
    )(h, wd, metas, lid)


def solution(mesh):
    n = round((mesh.shape["ep"] // 2) ** 0.5)

    def local(x, expert, slot, gate, w_gate, w_up, w_down):
        tokens, top = expert.shape[2:]
        experts = w_gate.shape[0] * mesh.shape["ep"]
        slots = 5 * tokens * top // (4 * experts)
        key = jnp.where(slot < slots, expert * slots + slot, -1)
        meta = jnp.concatenate([key[0, 0].T.astype(F32), gate[0, 0].T.astype(BF16).astype(F32)])
        c = rem(lax.axis_index("ep"), 2)
        lid = jnp.arange(4 * slots).reshape(2, 2, 1, slots)
        lid = jnp.where(c == 0, lid, lid[::-1]).astype(F32)
        up_lid = jnp.broadcast_to(lid.reshape(-1, 1), (4 * slots, tokens))
        none = jnp.full_like(lid, -experts * slots * 2)
        down_lid = jnp.stack([jnp.concatenate([lid, none], 2), jnp.concatenate([none, lid], 2)]).reshape(2, 1, -1)
        h, metas = up(n, slots, top, x[0, 0], meta, up_lid, w_gate, w_up)
        return down(n, slots, top, h, w_down, metas, down_lid)[None, None]

    tok, exp = P("dp", "ep", None, None), P("ep", None, None)
    return jax.shard_map(
        local, mesh=mesh, in_specs=(tok, tok, tok, tok, exp, exp, exp), out_specs=tok, check_vma=False
    )
```

```python
import functools

import jax
import jax.numpy as jnp
from jax import lax
from jax.experimental import pallas as pl
from jax.experimental.pallas import tpu as pltpu
from jax.sharding import PartitionSpec as P

MESH = pl.DeviceIdType.MESH
F32, BF16 = jnp.float32, jnp.bfloat16
UP, DOWN = 256, 256
KINDS = ((0, 0), (0, -1), (0, 1), (-1, 0), (-1, 1), (1, 0), (1, -1))
ROWS = (-1, 0, 1)
ROWS3 = (1, 2, 3)
TWO = range(2)
SIG = (1, -1)
FP, FM, SP, SM, HERE = (1, 0), (-1, 0), (0, 1), (0, -1), (0, 0)
OTHER, FAR = 1, 2
rem, div = lax.rem, lax.div


def kind(r, d):
    return KINDS.index((r, d))


def place(n):
    me = lax.axis_index("ep")
    c, chip = rem(me, 2), div(me, 2)
    a, b = div(chip, n), rem(chip, n)
    f, s = a * (1 - c) + b * c, b * (1 - c) + a * c

    def chip_at(at):
        ff, ss = rem(f + at[0] + n, n), rem(s + at[1] + n, n)
        return (ff * (1 - c) + ss * c) * n + ss * (1 - c) + ff * c

    def dev(at, other=0):
        return {"ep": chip_at(at) * 2 + (1 - c if other else c)}

    return dev, chip_at, c


def signal(sem, device):
    pl.semaphore_signal(sem, inc=1, device_id=device, device_id_type=MESH)


def greet(devices):
    barrier = pltpu.get_barrier_semaphore()
    for d in devices:
        signal(barrier, d)
    pl.semaphore_wait(barrier, len(devices))


def times(s, at=SP):
    return tuple(s * v for v in at)


def columns(j, h, width):
    return pl.ds(pl.multiple_of((2 * j + h) * width, width), width)


def dot(a, b):
    return jnp.dot(a, b, preferred_element_type=F32)


def up_kernel(
    n, chunks, top, x_ref, meta_ref, wg_ref, wu_ref, h_ref, near_ref,
    row, nxt, zbuf, leaf, rel, part, p_ref, metas, wbuf, acc, hst, send, recv, msend, mrecv, msem, xsem, wsem, hsem, cred,
):
    dev, chip_at, core = place(n)
    c40 = p_ref.shape[2] // 4
    w = n * c40
    partner = dev(HERE, OTHER)
    sources = [(df, ds) for df in range(n) for ds in ROWS if (df, ds) != HERE]
    greet([dev(at) for at in sources] + [dev(at, OTHER) for at in (FP, FM, SP, SM)] + [partner])

    def remote(src, dst, s, r, to):
        return pltpu.make_async_remote_copy(
            src_ref=src, dst_ref=dst, send_sem=s, recv_sem=r, device_id=to, device_id_type=MESH
        )

    def copy(i, j, src, dst, to):
        m = rem(j, 3)
        return remote(src, dst, send.at[m, i], recv.at[m, i], to)

    tell = [
        remote(meta_ref, metas.at[-df % n, 1 - ds], msend.at[i], mrecv.at[i], dev((df, ds)))
        for i, (df, ds) in enumerate(sources)
    ]
    own = pltpu.make_async_copy(meta_ref, metas.at[0, 1], msem.at[0])

    def ring(j):
        r = row.at[rem(j, 3)]
        return [copy(h, j, r.at[:, 0], r.at[:, -SIG[h] % n], dev(times(SIG[h], FP))) for h in TWO]

    def onward(j):
        r = row.at[rem(j, 3)]
        return [copy(2 + h, j, r.at[h, -SIG[h] % n], r.at[h, FAR], dev(times(SIG[h], FP))) for h in TWO]

    def raw(j):
        r, t = row.at[rem(j, 3)], nxt.at[rem(j, 3)]
        return [copy(4 + h, j, r.at[h], t.at[h], dev(times(SIG[h]))) for h in TWO]

    def leaves(j, h):
        z, q = zbuf.at[rem(j, 3)], leaf.at[rem(j, 2)]
        return [copy(6 + 2 * h + o, j, q.at[h, o], z.at[h, o, SIG[h] % n], dev(times(-SIG[h]), o)) for o in TWO]

    def relays(j, h):
        z, q = zbuf.at[rem(j, 3)], rel.at[rem(j, 2)]
        return [copy(10 + 2 * h + o, j, q.at[h, o], z.at[h, o, FAR], dev(times(SIG[h]), o)) for o in TWO]

    def mine(j):
        z, q = zbuf.at[rem(j, 3)], part.at[rem(j, 2)]
        return copy(14, j, q.at[0], z.at[:, 1, 0], partner)

    def mine_next(j, h):
        z, q = zbuf.at[rem(j, 3)], part.at[rem(j, 2)]
        return copy(15 + h, j, q.at[1, h], z.at[h, 1, -SIG[h] % n], partner)

    def load(j):
        r, s = row.at[rem(j, 3)], xsem.at[rem(j, 2)]
        return [pltpu.make_async_copy(x_ref.at[:, columns(j, h, UP)], r.at[h, 0], s.at[h]) for h in TWO]

    def weights(i, m, e):
        rows = pl.ds(pl.multiple_of(i * 2 * UP, UP), 2 * UP)
        return pltpu.make_async_copy((wg_ref, wu_ref)[m].at[e, rows], wbuf.at[m, e], wsem.at[m, e])

    def into_slots(kinds, src, puts):
        for pair in TWO:
            many = [jnp.concatenate([p_ref[k, 2 * pair + i] for k in kinds], axis=0) for i in TWO]
            r = [dot(many[i], src[2 * pair + i]) for i in TWO]
            for q, put in enumerate(puts):
                for o in TWO:
                    for e in TWO:
                        at = (4 * q + 2 * o + e) * c40
                        v = jnp.concatenate([x[at : at + c40] for x in r], axis=0).astype(BF16)
                        put(o, e, pl.ds(2 * pair * c40, 2 * c40), v)

    def matmul(i, m, e):
        weights(i, m, e).wait()
        z = zbuf.at[rem(i, 3)]
        a = jnp.concatenate([z[h, :, :, e].reshape(2 * n * w, UP) for h in TWO], axis=1)
        acc[m, e] += dot(a, wbuf[m, e]).reshape(acc.shape[2:])

        @pl.when(i + 1 < chunks)
        def _():
            weights(i + 1, m, e).start()

    for d in load(0) + [own] + tell:
        d.start()
    for m in TWO:
        for e in TWO:
            weights(0, m, e).start()

    def tables():
        own.wait()
        for d in tell:
            d.wait_recv()
        at = lax.broadcasted_iota(jnp.int32, p_ref.shape[2:], 0)
        swap = jnp.where(at < 2 * c40, 2 * c40, -2 * c40)
        lid = (at + swap * core).astype(F32)

        def source(g, carry):
            for k, (r, d) in enumerate(KINDS):
                first = (chip_at((0, d)) * 4 * c40).astype(F32)
                hit = None
                for j in range(top):
                    same = (metas[g, 1 + r, j : j + 1, :] - first) == lid
                    hit = same if hit is None else hit | same
                p_ref[k, g] = jnp.where(hit, 1.0, 0.0).astype(BF16)
            return carry

        lax.fori_loop(0, n, source, 0)
        for d in tell:
            d.wait_send()
        save = pltpu.make_async_copy(metas, near_ref, msem.at[1])
        save.start()
        save.wait()

    def step(k, carry):
        @pl.when(k >= 2)
        def _():
            for i in range(7):
                pl.semaphore_wait(cred.at[i], 1)

        @pl.when(k < chunks)
        def _():
            for d in load(k):
                d.wait()
            for d in ring(k):
                d.start()

        @pl.when(k + 1 < chunks)
        def _():
            for d in load(k + 1):
                d.start()

        j, i = k - 1, k - 2
        travels, multiplies = (k >= 1) & (k <= chunks), k >= 2

        @pl.when(travels)
        def _():

            @pl.when(k == 1)
            def _():
                tables()

            m3, m2 = rem(j, 3), rem(j, 2)
            for h in TWO:

                def out(o, e, rows, v):
                    leaf[m2, h, o, e, rows, :] = v

                def keep(o, e, rows, v):
                    if o == 0:
                        zbuf[m3, h, 0, 0, e, rows, :] = v
                    else:
                        part[m2, 0, h, e, rows, :] = v

                into_slots((kind(0, -SIG[h]), kind(*HERE)), row.at[m3, h], (out, keep))
                for d in leaves(j, h):
                    d.start()
            mine(j).start()

        @pl.when(k == 1)
        def _():
            acc[...] = jnp.zeros_like(acc)

        @pl.when(multiplies)
        def _():
            for h in TWO:
                for d in leaves(i, h) + relays(i, h) + [mine_next(i, h)]:
                    d.wait_recv()
            mine(i).wait_recv()
            matmul(i, 0, 0)

        @pl.when(k < chunks)
        def _():
            for d, e in zip(ring(k), onward(k)):
                d.wait_recv()
                e.start()

        @pl.when(multiplies)
        def _():
            matmul(i, 0, 1)

        @pl.when(travels)
        def _():
            m3, m2 = rem(j, 3), rem(j, 2)
            for h in TWO:
                raw(j)[h].wait_recv()

                def out(o, e, rows, v):
                    rel[m2, h, o, e, rows, :] = v

                def keep(o, e, rows, v):
                    if o == 0:
                        zbuf[m3, h, 0, -SIG[h] % n, e, rows, :] = v
                    else:
                        part[m2, 1, h, e, rows, :] = v

                into_slots((kind(-SIG[h], SIG[h]), kind(-SIG[h], 0)), nxt.at[m3, h], (out, keep))
                for d in relays(j, h):
                    d.start()
                mine_next(j, h).start()

        @pl.when(k < chunks)
        def _():
            for d in onward(k):
                d.wait_recv()
            for d in raw(k):
                d.start()

        @pl.when(multiplies)
        def _():
            for e in TWO:
                matmul(i, 1, e)

        @pl.when(travels)
        def _():
            for d in ring(j) + onward(j) + raw(j) + leaves(j, 0) + leaves(j, 1) + [mine(j)]:
                d.wait_send()

        @pl.when(multiplies)
        def _():
            for h in TWO:
                for d in relays(i, h) + [mine_next(i, h)]:
                    d.wait_send()

        @pl.when(k < chunks)
        def _():
            to = [dev(at) for at in (FM, FP, SM, SP)] + [dev(at, OTHER) for at in (FM, FP)] + [partner]
            for q, d in enumerate(to):
                signal(cred.at[q], d)

        return carry

    lax.fori_loop(0, chunks + 2, step, 0)

    def save(t):
        e, side, soff = div(t, 2 * n), div(rem(t, 2 * n), n), rem(t, n)
        return pltpu.make_async_copy(hst.at[rem(t, 2)], h_ref.at[e, side, soff], hsem.at[rem(t, 2)])

    blocks = 4 * n

    def gated(t, carry):
        e, side, soff = div(t, 2 * n), div(rem(t, 2 * n), n), rem(t, n)
        rows = pl.ds(pl.multiple_of(soff * w, w), w)

        @pl.when(t >= 2)
        def _():
            save(t - 2).wait()

        hst[rem(t, 2)] = (jax.nn.silu(acc[0, e, side, rows, :]) * acc[1, e, side, rows, :]).astype(BF16)
        save(t).start()
        return carry

    lax.fori_loop(0, blocks, gated, 0)
    for t in (blocks - 2, blocks - 1):
        save(t).wait()


def down_kernel(
    n, chunks, top, h_ref, wd_ref, metas, y_ref,
    hbuf, wbuf, c_ref, ob, orl, olf, opt, yrow, f2r, fr, yst, fst, fin, ysum, y0, yo, send, recv, wsem, hsem, ysem, cred,
):
    dev, chip_at, core = place(n)
    rows2 = c_ref.shape[3] // 4
    w = hbuf.shape[3]
    partner = dev(HERE, OTHER)
    greet([dev(at, o) for at in (FP, FM, SP, SM) for o in TWO] + [partner])

    def m4(j):
        return rem(j, 4)

    def copy(i, j, src, dst, to):
        m = m4(j)
        return pltpu.make_async_remote_copy(
            src_ref=src, dst_ref=dst, send_sem=send.at[m, i], recv_sem=recv.at[m, i], device_id=to, device_id_type=MESH
        )

    def to_relay(j, h):
        o, q = ob.at[m4(j)], orl.at[m4(j)]
        to = dev(times(-SIG[h])), dev(times(-SIG[h], FP), OTHER)
        return [copy(2 * v + h, j, o.at[h, v, FAR], q.at[h, v], to[v]) for v in TWO]

    def to_root(j, h):
        o, q = ob.at[m4(j)], olf.at[m4(j)]
        to = dev(times(SIG[h])), dev(times(SIG[h], FP), OTHER)
        return [copy(4 + 2 * v + h, j, o.at[h, v, SIG[h] % n], q.at[h, v], to[v]) for v in TWO]

    def mine(j, h):
        o, q = ob.at[m4(j)], opt.at[m4(j)]
        ends = ((0, 8 + h, 0), (1, 10 + h, -SIG[h] % n))
        return [copy(i, j, o.at[h, 1, s], q.at[v, h], partner) for v, i, s in ends]

    def relayed(j):
        return [copy(12 + h, j, yst.at[rem(j, 2), h], yrow.at[m4(j), h], dev(times(-SIG[h]))) for h in TWO]

    def far(j):
        return [copy(14 + h, j, fst.at[rem(j, 2), h], f2r.at[m4(j), h], dev(times(-SIG[h], FP))) for h in TWO]

    def near(j):
        return [copy(16 + h, j, fin.at[rem(j, 2), h], fr.at[m4(j), h], dev(times(-SIG[h], FP))) for h in TWO]

    def firsts(j):
        return [d for h in TWO for d in to_relay(j, h) + to_root(j, h) + mine(j, h)]

    def weights(j):
        b, s = wbuf.at[rem(j, 2)], wsem.at[rem(j, 2)]
        cols = pl.ds(pl.multiple_of(2 * j * DOWN, DOWN), 2 * DOWN)
        return [pltpu.make_async_copy(wd_ref.at[e, :, cols], b.at[e], s.at[e]) for e in TWO]

    def save(j):
        b = yo.at[rem(j, 2)]
        return [pltpu.make_async_copy(b.at[h], y_ref.at[:, columns(j, h, DOWN)], ysem.at[h]) for h in TWO]

    def hidden(e, side):
        return pltpu.make_async_copy(h_ref.at[e, side], hbuf.at[e, side], hsem.at[e, side])

    def tokens(k, pair, ours, theirs):
        cut = pl.ds(pair * rows2, rows2)
        v = jnp.concatenate([o[e, cut, :] for o in (ours, theirs) for e in TWO], axis=0)
        t = c_ref.shape[2]
        return dot(c_ref[k, 2 * pair : 2 * pair + 2].reshape(2 * t, c_ref.shape[3]), v).reshape(2, t, DOWN)

    for side in TWO:
        for e in TWO:
            hidden(e, side).start()
    for d in weights(0):
        d.start()

    def tables():
        at = lax.broadcasted_iota(jnp.int32, (1, c_ref.shape[3]), 1)
        q = sum((at >= rows2 * i).astype(jnp.int32) for i in ROWS3)
        at -= q * rows2
        second = (at >= rows2 // 2).astype(jnp.int32)
        slot = at - second * (rows2 // 2)
        expert = q + jnp.where(q < 2, 2, -2) * core

        def source(g, carry):
            lid = jnp.where(second == rem(g, 2), expert * (rows2 // 2) + slot, -(2**20)).astype(F32)
            for r in ROWS:
                meta = metas[g, 1 + r].T
                for d in ROWS:
                    if (r, d) in KINDS:
                        first = (chip_at((0, d)) * 2 * rows2).astype(F32)
                        v = jnp.zeros(c_ref.shape[2:], F32)
                        for j in range(top):
                            same = (meta[:, j : j + 1] - first) == lid
                            v = jnp.where(same, meta[:, top + j : top + j + 1], v)
                        c_ref[kind(r, d), g] = v.astype(BF16)
            return carry

        lax.fori_loop(0, n, source, 0)

    def step(k, carry):
        @pl.when(k >= 2)
        def _():
            for i in range(7):
                pl.semaphore_wait(cred.at[i], 1)

        @pl.when((k >= 3) & (k <= chunks + 2))
        def _():
            j = k - 3
            m, m2 = m4(j), rem(j, 2)
            for h in TWO:
                far(j)[h].wait_recv()
                g = 1 - h
                fin[m2, h, h] = (ysum[m2, h, g] + f2r[m, h].astype(F32)).astype(BF16)
                fin[m2, h, 1 - h] = ysum[m2, 1 - h, g].astype(BF16)
                near(j)[h].start()

        @pl.when((k >= 2) & (k <= chunks + 1))
        def _():
            j = k - 2
            m, m2 = m4(j), rem(j, 2)
            for d in to_root(j, 0) + to_root(j, 1) + [mine(j, h)[0] for h in TWO] + relayed(j):
                d.wait_recv()
            for h in TWO:
                s = SIG[h]
                for pair in (1, 0):
                    v = tokens(kind(*HERE), pair, ob.at[m, h, 0, 0], opt.at[m, 0, h])
                    v += tokens(kind(0, -s), pair, olf.at[m, h, 0], olf.at[m, h, 1])
                    v += yrow[m, h, 2 * pair : 2 * pair + 2].astype(F32)
                    ysum[m2, h, pair] = v[1]
                    if pair:
                        fst[m2, h] = v[0].astype(BF16)
                        far(j)[h].start()
                    else:
                        y0[m, h] = v[0]

        @pl.when((k >= 1) & (k <= chunks))
        def _():
            j = k - 1
            m = m4(j)
            for h in TWO:
                s = SIG[h]
                for d in to_relay(j, h) + mine(j, h)[1:]:
                    d.wait_recv()
                for pair in TWO:
                    v = tokens(kind(-s, 0), pair, ob.at[m, h, 0, -s % n], opt.at[m, 1, h])
                    v += tokens(kind(-s, s), pair, orl.at[m, h, 0], orl.at[m, h, 1])
                    yst[rem(j, 2), h, 2 * pair : 2 * pair + 2] = v.astype(BF16)
                relayed(j)[h].start()

        @pl.when(k + 1 < chunks)
        def _():
            for d in weights(k + 1):
                d.start()

        @pl.when(k < chunks)
        def _():
            for d in weights(k):
                d.wait()
            m = m4(k)
            for side in TWO:
                for e in TWO:

                    @pl.when(k == 0)
                    def _():
                        hidden(e, side).wait()

                    a = hbuf[e, side].reshape(n * w, hbuf.shape[4])
                    v = dot(a, wbuf[rem(k, 2), e]).astype(BF16)
                    for h in TWO:
                        ob[m, h, side, :, e] = v[:, h * DOWN : (h + 1) * DOWN].reshape(n, w, DOWN)
                for h in TWO:
                    to_relay(k, h)[side].start()
                    to_root(k, h)[side].start()
            for h in TWO:
                for d in mine(k, h):
                    d.start()

        @pl.when(k == 0)
        def _():
            tables()

        @pl.when(k >= 4)
        def _():
            j = k - 4
            m, m2 = m4(j), rem(j, 2)
            for d in near(j):
                d.wait_recv()
            for h in TWO:
                yo[m2, h] = (y0[m, h] + fr[m, 0, h].astype(F32) + fr[m, 1, h].astype(F32)).astype(BF16)
            for d in save(j):
                d.start()

        @pl.when((k >= 1) & (k <= chunks))
        def _():
            for d in firsts(k - 1):
                d.wait_send()

        @pl.when((k >= 2) & (k <= chunks + 1))
        def _():
            for d in relayed(k - 2):
                d.wait_send()

        @pl.when((k >= 3) & (k <= chunks + 2))
        def _():
            for d in far(k - 3):
                d.wait_send()

        @pl.when(k >= 4)
        def _():
            for d in near(k - 4):
                d.wait_send()
            for d in save(k - 4):
                d.wait()

        @pl.when(k < chunks + 2)
        def _():
            to = [dev(at) for at in (FM, FP, SM, SP)] + [dev(at, OTHER) for at in (SM, SP)] + [partner]
            for q, d in enumerate(to):
                signal(cred.at[q], d)

        return carry

    lax.fori_loop(0, chunks + 4, step, 0)


ANY = pl.BlockSpec(memory_space=pl.ANY)
VMEM = pl.BlockSpec(memory_space=pltpu.VMEM)
DMA, REGULAR = pltpu.SemaphoreType.DMA, pltpu.SemaphoreType.REGULAR


def bf16(*shape):
    return pltpu.VMEM(shape, BF16)


def f32(*shape):
    return pltpu.VMEM(shape, F32)


def params(i):
    return pltpu.CompilerParams(collective_id=i, has_side_effects=True, vmem_limit_bytes=66_500_000)


def up(n, slots, top, x, meta, wg, wu):
    t, d = x.shape
    w, ff = n * slots, wg.shape[-1]
    slot_rows = bf16(2, 2, 2, 2, w, UP)
    return pl.pallas_call(
        functools.partial(up_kernel, n, d // (2 * UP), top),
        out_shape=(
            jax.ShapeDtypeStruct((2, 2, n, w, ff), BF16),
            jax.ShapeDtypeStruct((n, len(ROWS), *meta.shape), F32),
        ),
        in_specs=[ANY, VMEM, ANY, ANY],
        out_specs=(ANY, ANY),
        scratch_shapes=[
            bf16(3, 2, n, t, UP),
            bf16(3, 2, n, t, UP),
            bf16(3, 2, 2, n, 2, w, UP),
            slot_rows,
            slot_rows,
            slot_rows,
            bf16(len(KINDS), n, 4 * slots, t),
            f32(n, len(ROWS), *meta.shape),
            bf16(2, 2, 2 * UP, ff),
            f32(2, 2, 2, n * w, ff),
            bf16(2, w, ff),
            DMA((3, 17)),
            DMA((3, 17)),
            DMA((3 * n - 1,)),
            DMA((3 * n - 1,)),
            DMA((2,)),
            DMA((2, 2)),
            DMA((2, 2)),
            DMA((2,)),
            REGULAR((7,)),
        ],
        compiler_params=params(0),
        name="up",
    )(x, meta, wg, wu)


def down(n, slots, top, h, wd, metas):
    d = wd.shape[-1]
    t, w, ff = metas.shape[-1], n * slots, h.shape[-1]
    rows = bf16(4, 2, 2, 2, w, DOWN)
    return pl.pallas_call(
        functools.partial(down_kernel, n, d // (2 * DOWN), top),
        out_shape=jax.ShapeDtypeStruct((t, d), BF16),
        in_specs=[ANY, ANY, VMEM],
        out_specs=ANY,
        scratch_shapes=[
            bf16(2, 2, n, w, ff),
            bf16(2, 2, ff, 2 * DOWN),
            bf16(len(KINDS), n, t, 8 * slots),
            bf16(4, 2, 2, n, 2, w, DOWN),
            rows,
            rows,
            rows,
            bf16(4, 2, n, t, DOWN),
            bf16(4, 2, t, DOWN),
            bf16(4, 2, 2, t, DOWN),
            bf16(2, 2, n, t, DOWN),
            bf16(2, 2, t, DOWN),
            bf16(2, 2, 2, t, DOWN),
            f32(2, 2, 2, t, DOWN),
            f32(4, 2, t, DOWN),
            bf16(2, 2, t, DOWN),
            DMA((4, 18)),
            DMA((4, 18)),
            DMA((2, 2)),
            DMA((2, 2)),
            DMA((2,)),
            REGULAR((7,)),
        ],
        compiler_params=params(1),
        name="down",
    )(h, wd, metas)


def solution(mesh):
    n = round((mesh.shape["ep"] // 2) ** 0.5)

    def local(x, expert, slot, gate, w_gate, w_up, w_down):
        tokens, top = expert.shape[2:]
        experts = w_gate.shape[0] * mesh.shape["ep"]
        slots = 5 * tokens * top // (4 * experts)
        key = jnp.where(slot < slots, expert * slots + slot, -1)
        meta = jnp.concatenate([key[0, 0].T.astype(F32), gate[0, 0].T.astype(BF16).astype(F32)])
        h, metas = up(n, slots, top, x[0, 0], meta, w_gate, w_up)
        return down(n, slots, top, h, w_down, metas)[None, None]

    tok, exp = P("dp", "ep", None, None), P("ep", None, None)
    return jax.shard_map(
        local, mesh=mesh, in_specs=(tok, tok, tok, tok, exp, exp, exp), out_specs=tok, check_vma=False
    )
```

```python
import functools

import jax
import jax.numpy as jnp
from jax import lax
from jax.experimental import pallas as pl
from jax.experimental.pallas import tpu as pltpu
from jax.sharding import PartitionSpec as P

MESH = pl.DeviceIdType.MESH
F32, BF16 = jnp.float32, jnp.bfloat16
UP, DOWN = 256, 256
KINDS = ((0, 0), (0, -1), (0, 1), (-1, 0), (-1, 1), (1, 0), (1, -1))
ROWS = (-1, 0, 1)
ROWS3 = (1, 2, 3)
TWO = range(2)
SIG = (1, -1)
FP, FM, SP, SM, HERE = (1, 0), (-1, 0), (0, 1), (0, -1), (0, 0)
OTHER, FAR = 1, 2
rem, div = lax.rem, lax.div


def kind(r, d):
    return KINDS.index((r, d))


def place(n):
    me = lax.axis_index("ep")
    c, chip = rem(me, 2), div(me, 2)
    a, b = div(chip, n), rem(chip, n)
    f, s = a * (1 - c) + b * c, b * (1 - c) + a * c

    def chip_at(at):
        ff, ss = rem(f + at[0] + n, n), rem(s + at[1] + n, n)
        return (ff * (1 - c) + ss * c) * n + ss * (1 - c) + ff * c

    def dev(at, other=0):
        return {"ep": chip_at(at) * 2 + (1 - c if other else c)}

    return dev, chip_at, c


def signal(sem, device):
    pl.semaphore_signal(sem, inc=1, device_id=device, device_id_type=MESH)


def greet(devices):
    barrier = pltpu.get_barrier_semaphore()
    for d in devices:
        signal(barrier, d)
    pl.semaphore_wait(barrier, len(devices))


def times(s, at=SP):
    return tuple(s * v for v in at)


def columns(j, h, width):
    return pl.ds(pl.multiple_of((2 * j + h) * width, width), width)


def dot(a, b):
    return jnp.dot(a, b, preferred_element_type=F32)


def up_kernel(
    n, chunks, top, x_ref, meta_ref, wg_ref, wu_ref, h_ref, near_ref,
    row, nxt, zbuf, leaf, rel, part, p_ref, metas, wbuf, acc, hst, send, recv, msend, mrecv, msem, xsem, wsem, hsem, cred,
):
    dev, chip_at, core = place(n)
    c40 = p_ref.shape[2] // 4
    w = n * c40
    partner = dev(HERE, OTHER)
    sources = [(df, ds) for df in range(n) for ds in ROWS if (df, ds) != HERE]
    greet([dev(at) for at in sources] + [dev(at, OTHER) for at in (FP, FM, SP, SM)] + [partner])

    def remote(src, dst, s, r, to):
        return pltpu.make_async_remote_copy(
            src_ref=src, dst_ref=dst, send_sem=s, recv_sem=r, device_id=to, device_id_type=MESH
        )

    def copy(i, j, src, dst, to):
        m = rem(j, 3)
        return remote(src, dst, send.at[m, i], recv.at[m, i], to)

    tell = [
        remote(meta_ref, metas.at[-df % n, 1 - ds], msend.at[i], mrecv.at[i], dev((df, ds)))
        for i, (df, ds) in enumerate(sources)
    ]
    own = pltpu.make_async_copy(meta_ref, metas.at[0, 1], msem.at[0])

    def ring(j):
        r = row.at[rem(j, 3)]
        return [copy(h, j, r.at[:, 0], r.at[:, -SIG[h] % n], dev(times(SIG[h], FP))) for h in TWO]

    def onward(j):
        r = row.at[rem(j, 3)]
        return [copy(2 + h, j, r.at[h, -SIG[h] % n], r.at[h, FAR], dev(times(SIG[h], FP))) for h in TWO]

    def raw(j):
        r, t = row.at[rem(j, 3)], nxt.at[rem(j, 3)]
        return [copy(4 + h, j, r.at[h], t.at[h], dev(times(SIG[h]))) for h in TWO]

    def leaves(j, h):
        z, q = zbuf.at[rem(j, 3)], leaf.at[rem(j, 2)]
        return [copy(6 + 2 * h + o, j, q.at[h, o], z.at[h, o, SIG[h] % n], dev(times(-SIG[h]), o)) for o in TWO]

    def relays(j, h):
        z, q = zbuf.at[rem(j, 3)], rel.at[rem(j, 2)]
        return [copy(10 + 2 * h + o, j, q.at[h, o], z.at[h, o, FAR], dev(times(SIG[h]), o)) for o in TWO]

    def mine(j):
        z, q = zbuf.at[rem(j, 3)], part.at[rem(j, 2)]
        return copy(14, j, q.at[0], z.at[:, 1, 0], partner)

    def mine_next(j, h):
        z, q = zbuf.at[rem(j, 3)], part.at[rem(j, 2)]
        return copy(15 + h, j, q.at[1, h], z.at[h, 1, -SIG[h] % n], partner)

    def load(j):
        r, s = row.at[rem(j, 3)], xsem.at[rem(j, 2)]
        return [pltpu.make_async_copy(x_ref.at[:, columns(j, h, UP)], r.at[h, 0], s.at[h]) for h in TWO]

    def weights(i, m, e):
        rows = pl.ds(pl.multiple_of(i * 2 * UP, UP), 2 * UP)
        return pltpu.make_async_copy((wg_ref, wu_ref)[m].at[e, rows], wbuf.at[m, e], wsem.at[m, e])

    def into_slots(kinds, src, puts):
        for pair in TWO:
            many = [jnp.concatenate([p_ref[k, 2 * pair + i] for k in kinds], axis=0) for i in TWO]
            r = [dot(many[i], src[2 * pair + i]) for i in TWO]
            for q, put in enumerate(puts):
                for o in TWO:
                    for e in TWO:
                        at = (4 * q + 2 * o + e) * c40
                        v = jnp.concatenate([x[at : at + c40] for x in r], axis=0).astype(BF16)
                        put(o, e, pl.ds(2 * pair * c40, 2 * c40), v)

    def matmul(i, m, e):
        weights(i, m, e).wait()
        z = zbuf.at[rem(i, 3)]
        a = jnp.concatenate([z[h, :, :, e].reshape(2 * n * w, UP) for h in TWO], axis=1)
        acc[m, e] += dot(a, wbuf[m, e]).reshape(acc.shape[2:])

        @pl.when(i + 1 < chunks)
        def _():
            weights(i + 1, m, e).start()

    for d in load(0) + [own] + tell:
        d.start()
    for m in TWO:
        for e in TWO:
            weights(0, m, e).start()

    def tables():
        own.wait()
        for d in tell:
            d.wait_recv()
        at = lax.broadcasted_iota(jnp.int32, p_ref.shape[2:], 0)
        swap = jnp.where(at < 2 * c40, 2 * c40, -2 * c40)
        lid = (at + swap * core).astype(F32)

        def source(g, carry):
            for k, (r, d) in enumerate(KINDS):
                first = (chip_at((0, d)) * 4 * c40).astype(F32)
                hit = None
                for j in range(top):
                    same = (metas[g, 1 + r, j : j + 1, :] - first) == lid
                    hit = same if hit is None else hit | same
                p_ref[k, g] = jnp.where(hit, 1.0, 0.0).astype(BF16)
            return carry

        lax.fori_loop(0, n, source, 0)
        for d in tell:
            d.wait_send()
        save = pltpu.make_async_copy(metas, near_ref, msem.at[1])
        save.start()
        save.wait()

    def step(k, carry):
        @pl.when(k >= 2)
        def _():
            for i in range(7):
                pl.semaphore_wait(cred.at[i], 1)

        @pl.when(k < chunks)
        def _():
            for d in load(k):
                d.wait()
            for d in ring(k):
                d.start()

        @pl.when(k + 1 < chunks)
        def _():
            for d in load(k + 1):
                d.start()

        j, i = k - 1, k - 2
        travels, multiplies = (k >= 1) & (k <= chunks), k >= 2

        @pl.when(travels)
        def _():

            @pl.when(k == 1)
            def _():
                tables()

            m3, m2 = rem(j, 3), rem(j, 2)
            for h in TWO:

                def out(o, e, rows, v):
                    leaf[m2, h, o, e, rows, :] = v

                def keep(o, e, rows, v):
                    if o == 0:
                        zbuf[m3, h, 0, 0, e, rows, :] = v
                    else:
                        part[m2, 0, h, e, rows, :] = v

                into_slots((kind(0, -SIG[h]), kind(*HERE)), row.at[m3, h], (out, keep))
                for d in leaves(j, h):
                    d.start()
            mine(j).start()

        @pl.when(k == 1)
        def _():
            acc[...] = jnp.zeros_like(acc)

        @pl.when(multiplies)
        def _():
            for h in TWO:
                for d in leaves(i, h) + relays(i, h) + [mine_next(i, h)]:
                    d.wait_recv()
            mine(i).wait_recv()
            matmul(i, 0, 0)

        @pl.when(k < chunks)
        def _():
            for d, e in zip(ring(k), onward(k)):
                d.wait_recv()
                e.start()

        @pl.when(multiplies)
        def _():
            matmul(i, 0, 1)

        @pl.when(travels)
        def _():
            m3, m2 = rem(j, 3), rem(j, 2)
            for h in TWO:
                raw(j)[h].wait_recv()

                def out(o, e, rows, v):
                    rel[m2, h, o, e, rows, :] = v

                def keep(o, e, rows, v):
                    if o == 0:
                        zbuf[m3, h, 0, -SIG[h] % n, e, rows, :] = v
                    else:
                        part[m2, 1, h, e, rows, :] = v

                into_slots((kind(-SIG[h], SIG[h]), kind(-SIG[h], 0)), nxt.at[m3, h], (out, keep))
                for d in relays(j, h):
                    d.start()
                mine_next(j, h).start()

        @pl.when(k < chunks)
        def _():
            for d in onward(k):
                d.wait_recv()
            for d in raw(k):
                d.start()

        @pl.when(multiplies)
        def _():
            for e in TWO:
                matmul(i, 1, e)

        @pl.when(travels)
        def _():
            for d in ring(j) + onward(j) + raw(j) + leaves(j, 0) + leaves(j, 1) + [mine(j)]:
                d.wait_send()

        @pl.when(multiplies)
        def _():
            for h in TWO:
                for d in relays(i, h) + [mine_next(i, h)]:
                    d.wait_send()

        @pl.when(k < chunks)
        def _():
            to = [dev(at) for at in (FM, FP, SM, SP)] + [dev(at, OTHER) for at in (FM, FP)] + [partner]
            for q, d in enumerate(to):
                signal(cred.at[q], d)

        return carry

    lax.fori_loop(0, chunks + 2, step, 0)

    def save(t):
        e, side, soff = div(t, 2 * n), div(rem(t, 2 * n), n), rem(t, n)
        return pltpu.make_async_copy(hst.at[rem(t, 2)], h_ref.at[e, side, soff], hsem.at[rem(t, 2)])

    blocks = 4 * n

    def gated(t, carry):
        e, side, soff = div(t, 2 * n), div(rem(t, 2 * n), n), rem(t, n)
        rows = pl.ds(pl.multiple_of(soff * w, w), w)

        @pl.when(t >= 2)
        def _():
            save(t - 2).wait()

        hst[rem(t, 2)] = (jax.nn.silu(acc[0, e, side, rows, :]) * acc[1, e, side, rows, :]).astype(BF16)
        save(t).start()
        return carry

    lax.fori_loop(0, blocks, gated, 0)
    for t in (blocks - 2, blocks - 1):
        save(t).wait()


def down_kernel(
    n, chunks, top, h_ref, wd_ref, metas, y_ref,
    hbuf, wbuf, c_ref, ob, orl, olf, opt, yrow, f2r, fr, yst, fst, fin, ysum, y0, yo, send, recv, wsem, hsem, ysem, cred,
):
    dev, chip_at, core = place(n)
    rows2 = c_ref.shape[3] // 4
    w = hbuf.shape[3]
    partner = dev(HERE, OTHER)
    greet([dev(at, o) for at in (FP, FM, SP, SM) for o in TWO] + [partner])

    def m4(j):
        return rem(j, 4)

    def copy(i, j, src, dst, to):
        m = m4(j)
        return pltpu.make_async_remote_copy(
            src_ref=src, dst_ref=dst, send_sem=send.at[m, i], recv_sem=recv.at[m, i], device_id=to, device_id_type=MESH
        )

    def to_relay(j, h):
        o, q = ob.at[m4(j)], orl.at[m4(j)]
        to = dev(times(-SIG[h])), dev(times(-SIG[h], FP), OTHER)
        return [copy(2 * v + h, j, o.at[h, v, FAR], q.at[h, v], to[v]) for v in TWO]

    def to_root(j, h):
        o, q = ob.at[m4(j)], olf.at[m4(j)]
        to = dev(times(SIG[h])), dev(times(SIG[h], FP), OTHER)
        return [copy(4 + 2 * v + h, j, o.at[h, v, SIG[h] % n], q.at[h, v], to[v]) for v in TWO]

    def mine(j, h):
        o, q = ob.at[m4(j)], opt.at[m4(j)]
        ends = ((0, 8 + h, 0), (1, 10 + h, -SIG[h] % n))
        return [copy(i, j, o.at[h, 1, s], q.at[v, h], partner) for v, i, s in ends]

    def relayed(j):
        return [copy(12 + h, j, yst.at[rem(j, 2), h], yrow.at[m4(j), h], dev(times(-SIG[h]))) for h in TWO]

    def far(j):
        return [copy(14 + h, j, fst.at[rem(j, 2), h], f2r.at[m4(j), h], dev(times(-SIG[h], FP))) for h in TWO]

    def near(j):
        return [copy(16 + h, j, fin.at[rem(j, 2), h], fr.at[m4(j), h], dev(times(-SIG[h], FP))) for h in TWO]

    def firsts(j):
        return [d for h in TWO for d in to_relay(j, h) + to_root(j, h) + mine(j, h)]

    def weights(j):
        b, s = wbuf.at[rem(j, 2)], wsem.at[rem(j, 2)]
        cols = pl.ds(pl.multiple_of(2 * j * DOWN, DOWN), 2 * DOWN)
        return [pltpu.make_async_copy(wd_ref.at[e, :, cols], b.at[e], s.at[e]) for e in TWO]

    def save(j):
        b = yo.at[rem(j, 2)]
        return [pltpu.make_async_copy(b.at[h], y_ref.at[:, columns(j, h, DOWN)], ysem.at[h]) for h in TWO]

    def hidden(e, side):
        return pltpu.make_async_copy(h_ref.at[e, side], hbuf.at[e, side], hsem.at[e, side])

    def tokens(k, pair, ours, theirs):
        cut = pl.ds(pair * rows2, rows2)
        v = jnp.concatenate([o[e, cut, :] for o in (ours, theirs) for e in TWO], axis=0)
        t = c_ref.shape[2]
        return dot(c_ref[k, 2 * pair : 2 * pair + 2].reshape(2 * t, c_ref.shape[3]), v).reshape(2, t, DOWN)

    for side in TWO:
        for e in TWO:
            hidden(e, side).start()
    for d in weights(0):
        d.start()

    def tables(sources):
        at = lax.broadcasted_iota(jnp.int32, (1, c_ref.shape[3]), 1)
        q = sum((at >= rows2 * i).astype(jnp.int32) for i in ROWS3)
        at -= q * rows2
        second = (at >= rows2 // 2).astype(jnp.int32)
        slot = at - second * (rows2 // 2)
        expert = q + jnp.where(q < 2, 2, -2) * core

        def source(g, carry):
            lid = jnp.where(second == rem(g, 2), expert * (rows2 // 2) + slot, -(2**20)).astype(F32)
            for r in sources:
                meta = metas[g, 1 + r].T
                for d in ROWS:
                    if (r, d) in KINDS:
                        first = (chip_at((0, d)) * 2 * rows2).astype(F32)
                        v = jnp.zeros(c_ref.shape[2:], F32)
                        for j in range(top):
                            same = (meta[:, j : j + 1] - first) == lid
                            v = jnp.where(same, meta[:, top + j : top + j + 1], v)
                        c_ref[kind(r, d), g] = v.astype(BF16)
            return carry

        lax.fori_loop(0, n, source, 0)

    def step(k, carry):
        @pl.when(k >= 2)
        def _():
            for i in range(7):
                pl.semaphore_wait(cred.at[i], 1)

        @pl.when((k >= 3) & (k <= chunks + 2))
        def _():
            j = k - 3
            m, m2 = m4(j), rem(j, 2)
            for h in TWO:
                far(j)[h].wait_recv()
                g = 1 - h
                fin[m2, h, h] = (ysum[m2, h, g] + f2r[m, h].astype(F32)).astype(BF16)
                fin[m2, h, 1 - h] = ysum[m2, 1 - h, g].astype(BF16)
                near(j)[h].start()

        @pl.when((k >= 2) & (k <= chunks + 1))
        def _():
            j = k - 2
            m, m2 = m4(j), rem(j, 2)
            for d in to_root(j, 0) + to_root(j, 1) + [mine(j, h)[0] for h in TWO] + relayed(j):
                d.wait_recv()
            for h in TWO:
                s = SIG[h]
                for pair in (1, 0):
                    v = tokens(kind(*HERE), pair, ob.at[m, h, 0, 0], opt.at[m, 0, h])
                    v += tokens(kind(0, -s), pair, olf.at[m, h, 0], olf.at[m, h, 1])
                    v += yrow[m, h, 2 * pair : 2 * pair + 2].astype(F32)
                    ysum[m2, h, pair] = v[1]
                    if pair:
                        fst[m2, h] = v[0].astype(BF16)
                        far(j)[h].start()
                    else:
                        y0[m, h] = v[0]

        @pl.when((k >= 1) & (k <= chunks))
        def _():
            j = k - 1
            m = m4(j)
            for h in TWO:
                s = SIG[h]
                for d in to_relay(j, h) + mine(j, h)[1:]:
                    d.wait_recv()
                for pair in TWO:
                    v = tokens(kind(-s, 0), pair, ob.at[m, h, 0, -s % n], opt.at[m, 1, h])
                    v += tokens(kind(-s, s), pair, orl.at[m, h, 0], orl.at[m, h, 1])
                    yst[rem(j, 2), h, 2 * pair : 2 * pair + 2] = v.astype(BF16)
                relayed(j)[h].start()

        @pl.when(k + 1 < chunks)
        def _():
            for d in weights(k + 1):
                d.start()

        @pl.when(k < chunks)
        def _():
            for d in weights(k):
                d.wait()
            m = m4(k)
            for side in TWO:
                for e in TWO:

                    @pl.when(k == 0)
                    def _():
                        hidden(e, side).wait()

                    a = hbuf[e, side].reshape(n * w, hbuf.shape[4])
                    v = dot(a, wbuf[rem(k, 2), e]).astype(BF16)
                    for h in TWO:
                        ob[m, h, side, :, e] = v[:, h * DOWN : (h + 1) * DOWN].reshape(n, w, DOWN)
                for h in TWO:
                    to_relay(k, h)[side].start()
                    to_root(k, h)[side].start()
            for h in TWO:
                for d in mine(k, h):
                    d.start()

        @pl.when(k == 0)
        def _():
            tables(SIG)

        @pl.when(k == 1)
        def _():
            tables((0,))

        @pl.when(k >= 4)
        def _():
            j = k - 4
            m, m2 = m4(j), rem(j, 2)
            for d in near(j):
                d.wait_recv()
            for h in TWO:
                yo[m2, h] = (y0[m, h] + fr[m, 0, h].astype(F32) + fr[m, 1, h].astype(F32)).astype(BF16)
            for d in save(j):
                d.start()

        @pl.when((k >= 1) & (k <= chunks))
        def _():
            for d in firsts(k - 1):
                d.wait_send()

        @pl.when((k >= 2) & (k <= chunks + 1))
        def _():
            for d in relayed(k - 2):
                d.wait_send()

        @pl.when((k >= 3) & (k <= chunks + 2))
        def _():
            for d in far(k - 3):
                d.wait_send()

        @pl.when(k >= 4)
        def _():
            for d in near(k - 4):
                d.wait_send()
            for d in save(k - 4):
                d.wait()

        @pl.when(k < chunks + 2)
        def _():
            to = [dev(at) for at in (FM, FP, SM, SP)] + [dev(at, OTHER) for at in (SM, SP)] + [partner]
            for q, d in enumerate(to):
                signal(cred.at[q], d)

        return carry

    lax.fori_loop(0, chunks + 4, step, 0)


ANY = pl.BlockSpec(memory_space=pl.ANY)
VMEM = pl.BlockSpec(memory_space=pltpu.VMEM)
DMA, REGULAR = pltpu.SemaphoreType.DMA, pltpu.SemaphoreType.REGULAR


def bf16(*shape):
    return pltpu.VMEM(shape, BF16)


def f32(*shape):
    return pltpu.VMEM(shape, F32)


def params(i):
    return pltpu.CompilerParams(collective_id=i, has_side_effects=True, vmem_limit_bytes=66_500_000)


def up(n, slots, top, x, meta, wg, wu):
    t, d = x.shape
    w, ff = n * slots, wg.shape[-1]
    slot_rows = bf16(2, 2, 2, 2, w, UP)
    return pl.pallas_call(
        functools.partial(up_kernel, n, d // (2 * UP), top),
        out_shape=(
            jax.ShapeDtypeStruct((2, 2, n, w, ff), BF16),
            jax.ShapeDtypeStruct((n, len(ROWS), *meta.shape), F32),
        ),
        in_specs=[ANY, VMEM, ANY, ANY],
        out_specs=(ANY, ANY),
        scratch_shapes=[
            bf16(3, 2, n, t, UP),
            bf16(3, 2, n, t, UP),
            bf16(3, 2, 2, n, 2, w, UP),
            slot_rows,
            slot_rows,
            slot_rows,
            bf16(len(KINDS), n, 4 * slots, t),
            f32(n, len(ROWS), *meta.shape),
            bf16(2, 2, 2 * UP, ff),
            f32(2, 2, 2, n * w, ff),
            bf16(2, w, ff),
            DMA((3, 17)),
            DMA((3, 17)),
            DMA((3 * n - 1,)),
            DMA((3 * n - 1,)),
            DMA((2,)),
            DMA((2, 2)),
            DMA((2, 2)),
            DMA((2,)),
            REGULAR((7,)),
        ],
        compiler_params=params(0),
        name="up",
    )(x, meta, wg, wu)


def down(n, slots, top, h, wd, metas):
    d = wd.shape[-1]
    t, w, ff = metas.shape[-1], n * slots, h.shape[-1]
    rows = bf16(4, 2, 2, 2, w, DOWN)
    return pl.pallas_call(
        functools.partial(down_kernel, n, d // (2 * DOWN), top),
        out_shape=jax.ShapeDtypeStruct((t, d), BF16),
        in_specs=[ANY, ANY, VMEM],
        out_specs=ANY,
        scratch_shapes=[
            bf16(2, 2, n, w, ff),
            bf16(2, 2, ff, 2 * DOWN),
            bf16(len(KINDS), n, t, 8 * slots),
            bf16(4, 2, 2, n, 2, w, DOWN),
            rows,
            rows,
            rows,
            bf16(4, 2, n, t, DOWN),
            bf16(4, 2, t, DOWN),
            bf16(4, 2, 2, t, DOWN),
            bf16(2, 2, n, t, DOWN),
            bf16(2, 2, t, DOWN),
            bf16(2, 2, 2, t, DOWN),
            f32(2, 2, 2, t, DOWN),
            f32(4, 2, t, DOWN),
            bf16(2, 2, t, DOWN),
            DMA((4, 18)),
            DMA((4, 18)),
            DMA((2, 2)),
            DMA((2, 2)),
            DMA((2,)),
            REGULAR((7,)),
        ],
        compiler_params=params(1),
        name="down",
    )(h, wd, metas)


def solution(mesh):
    n = round((mesh.shape["ep"] // 2) ** 0.5)

    def local(x, expert, slot, gate, w_gate, w_up, w_down):
        tokens, top = expert.shape[2:]
        experts = w_gate.shape[0] * mesh.shape["ep"]
        slots = 5 * tokens * top // (4 * experts)
        key = jnp.where(slot < slots, expert * slots + slot, -1)
        meta = jnp.concatenate([key[0, 0].T.astype(F32), gate[0, 0].T.astype(BF16).astype(F32)])
        h, metas = up(n, slots, top, x[0, 0], meta, w_gate, w_up)
        return down(n, slots, top, h, w_down, metas)[None, None]

    tok, exp = P("dp", "ep", None, None), P("ep", None, None)
    return jax.shard_map(
        local, mesh=mesh, in_specs=(tok, tok, tok, tok, exp, exp, exp), out_specs=tok, check_vma=False
    )
```
